32 devices in a mesh: groups: 2 (over x), samp: 16 (over z, y, core).
Axes of the slice: x: 2, y: 2, z: 4, core: 2. Of those that a mesh axis runs over, the one named last changes fastest.
Arguments:
- dosage: bfloat16 [8192, 8192], P(('groups', 'samp')), parts along dimension 0, may hold values from 0 to 2
- covariates: bfloat16 [8192, 96], P(('groups', 'samp')), parts along dimension 0, may hold values from -8 to 8
- expression: bfloat16 [8192, 8192], P('groups', 'samp'), parts along dimension 0, may hold values from -10 to 10
- block_index: int32 [4, 1024], P('groups'), parts along dimension 0, may hold values from 0 to 8191
- expr_row: int32 [8192], P('groups'), parts along dimension 0, may hold values from 0 to 4095, each once
Outputs:
- zscore: float32 [4096, 8192], P('groups', 'samp'), parts along dimension 0
The draws below stay inside these ranges and needn't reach their ends.
There are 2 independent parts, one for each index of `groups`. The reference program is written for one: setup_inputs(seed, part) draws one part's arguments, and reference() takes and returns one part's arrays. A program takes and returns all parts, laid end to end along the dimension named above; each array names one. Nothing has to cross between parts.
Inputs may be any that keep to these rules, and one draw needn't show every extreme that they name: `expr_row`: every expression row appears once.
All inputs are finite; a program needn't handle non-finite values.
Results may differ from the reference program's by a relative error of at most 0.0029.
Values may be sent and summed in bfloat16 or wider, within the bound.
No kernel may reach another device: no remote copies, remote signals or barrier semaphores. Data moves between devices by JAX's collectives and lax.ppermute only.
A program may use at most 192 MiB of HBM per device.

```python
import math
import jax
import jax.numpy as jnp
from jax import lax

K = 96
V = 1024
BLOCKS = 2
VPANEL = 8192
NSAMP = 4096
GENES = 8192


def covariate_base(key):
    first = jax.random.fold_in(key, 11)
    normal_part = jax.random.normal(first, (NSAMP, K), jnp.float32)
    rising = 1.0 + 2.0 * jnp.arange(NSAMP, dtype=jnp.float32) / NSAMP
    return jnp.clip(normal_part * rising[:, None], -8.0, 8.0)


def draw_covariates(key, part):
    return covariate_base(key).astype(jnp.bfloat16)


def draw_dosage(key, part):
    base = covariate_base(key)
    loading = jax.random.normal(jax.random.fold_in(key, 21), (K, VPANEL), jnp.float32)
    noise_key = jax.random.fold_in(key, 22)
    noise = jax.random.uniform(noise_key, (NSAMP, VPANEL), jnp.float32, -0.6, 0.6)
    shared = jnp.dot(base, loading) * (0.3 / K ** 0.5)
    return jnp.clip(1.0 + shared + noise, 0.0, 2.0).astype(jnp.bfloat16)


def draw_expression(key, part):
    base = covariate_base(key)
    loading = jax.random.normal(jax.random.fold_in(key, 31), (K, GENES), jnp.float32)
    noise_key = jax.random.fold_in(key, 32)
    noise = jax.random.normal(noise_key, (NSAMP, GENES), jnp.float32)
    shared = jnp.dot(base, loading) * (0.5 / K ** 0.5)
    return jnp.clip(shared + noise, -10.0, 10.0).astype(jnp.bfloat16)


def plant(entries, own_key, least, high):
    place = [jax.random.randint(jax.random.fold_in(own_key, axis), (), 0, length) for axis, length in enumerate(entries.shape)]
    widest = entries.shape.index(max(entries.shape))
    beside = place[:widest] + [(place[widest] + 1) % entries.shape[widest]] + place[widest + 1:]
    return entries.at[tuple(place)].set(least).at[tuple(beside)].set(high)


def setup_inputs(seed: int = 0, part: int = 0) -> dict:
    key_list = jax.random.split(jax.random.key(seed), 6)
    part_keys = jax.random.split(jax.random.fold_in(key_list[5], part), 6)
    dosage = draw_dosage(jax.random.fold_in(jax.random.fold_in(key_list[5], part), 71), part)
    covariates = draw_covariates(jax.random.fold_in(jax.random.fold_in(key_list[5], part), 71), part)
    expression = draw_expression(jax.random.fold_in(jax.random.fold_in(key_list[5], part), 71), part)
    block_index = plant(jax.random.randint(part_keys[3], (BLOCKS, V), 0, VPANEL), jax.random.fold_in(part_keys[3], 1), 0, VPANEL - 1).astype(jnp.int32)
    expr_row = jax.random.permutation(part_keys[4], NSAMP).astype(jnp.int32)
    return dict(dosage=dosage, covariates=covariates, expression=expression, block_index=block_index, expr_row=expr_row)


epsilon = 1e-06

def reference(dosage, covariates, expression, block_index, expr_row):
    gram = jnp.dot(covariates.T.astype(jnp.float32), covariates.astype(jnp.float32), preferred_element_type=jnp.float32)
    factor = jnp.linalg.cholesky(gram)
    matched = jnp.take(expression, expr_row, axis=0)
    panel_norm = lax.optimization_barrier(jnp.sum(jnp.square(expression.astype(jnp.float32)), axis=0))
    cov_float = covariates.astype(jnp.float32)
    scale = math.sqrt(NSAMP - K - 1)
    results = []
    for block in range(BLOCKS):
        picked = jnp.take(dosage, block_index[block], axis=1)
        loads = jnp.dot(covariates.T.astype(jnp.float32), picked.astype(jnp.float32), preferred_element_type=jnp.float32)
        coeffs = jax.scipy.linalg.cho_solve((factor, True), loads)
        fitted = jnp.dot(cov_float, coeffs, precision=lax.Precision.HIGHEST)
        resid = (picked.astype(jnp.float32) - fitted).astype(jnp.bfloat16)
        resid_norm = lax.optimization_barrier(jnp.sum(jnp.square(resid.astype(jnp.float32)), axis=0))
        products = jnp.dot(resid.T.astype(jnp.float32), matched.astype(jnp.float32), preferred_element_type=jnp.float32)
        results.append(scale * products * lax.rsqrt(resid_norm + epsilon)[:, None] * lax.rsqrt(panel_norm + epsilon)[None, :])
    return jnp.concatenate(results, axis=0)
```

```python
import functools
import math

import jax
import jax.numpy as jnp
from jax import lax
from jax.experimental import pallas as pl
from jax.experimental.pallas import tpu as pltpu
from jax.sharding import PartitionSpec as P

epsilon = 1e-06
LANES = 128


def dot32(a, b):
    return jnp.dot(a, b, preferred_element_type=jnp.float32)


def gather_rows(dst, src, idx_ref, base, rows, nl, unroll=32):
    def body(j, _):
        first = pl.multiple_of(j * unroll, unroll)
        for u in range(unroll):
            i = idx_ref[base + first + u]
            dst[pl.ds(pl.multiple_of((first + u) * nl, nl), nl), :] = src[
                pl.ds(pl.multiple_of(i * nl, nl), nl), :
            ]
        return 0

    lax.fori_loop(0, rows // unroll, body, 0)


def pick_kernel(idx_ref, x_ref, o_ref, t_ref, g_ref):
    rows, n = x_ref.shape
    nl = rows // LANES
    width = o_ref.shape[0]
    step = 1024
    for k in range(0, n, step):
        v = x_ref[:, k : k + step].astype(jnp.float32).T
        for l in range(nl):
            t_ref[pl.ds(k * nl + l, step, stride=nl), :] = v[:, l * LANES : (l + 1) * LANES]
    gather_rows(g_ref, t_ref, idx_ref, 0, width, nl)
    for l in range(nl):
        o_ref[:, l * LANES : (l + 1) * LANES] = g_ref[pl.ds(l, width, stride=nl), :].astype(
            jnp.bfloat16
        )


def pick(x, idx):
    rows, n = x.shape
    (width,) = idx.shape
    nl = rows // LANES
    return pl.pallas_call(
        pick_kernel,
        grid_spec=pltpu.PrefetchScalarGridSpec(
            num_scalar_prefetch=1,
            grid=(1,),
            in_specs=[pl.BlockSpec((rows, n), lambda b, i: (0, 0))],
            out_specs=pl.BlockSpec((width, rows), lambda b, i: (0, 0)),
            scratch_shapes=[
                pltpu.VMEM((n * nl, LANES), jnp.float32),
                pltpu.VMEM((width * nl, LANES), jnp.float32),
            ],
        ),
        out_shape=jax.ShapeDtypeStruct((width, rows), jnp.bfloat16),
        name="pick",
    )(idx, x)


def match_kernel(idx_ref, e_ref, o_ref, norm_ref, f_ref, g_ref):
    b = pl.program_id(0)
    n, genes = e_ref.shape
    rows = o_ref.shape[0]
    nl = genes // LANES

    @pl.when(b == 0)
    def _():
        step = 512
        total = jnp.zeros((8, genes), jnp.float32)
        for k in range(0, n, step):
            v = e_ref[k : k + step, :].astype(jnp.float32)
            for l in range(nl):
                f_ref[pl.ds(k * nl + l, step, stride=nl), :] = v[:, l * LANES : (l + 1) * LANES]
            total = total + jnp.sum((v * v).reshape(step // 8, 8, genes), axis=0)
        norm_ref[...] = jnp.sum(total, axis=0, keepdims=True)

    gather_rows(g_ref, f_ref, idx_ref, b * rows, rows, nl)
    for l in range(nl):
        o_ref[:, l * LANES : (l + 1) * LANES] = g_ref[pl.ds(l, rows, stride=nl), :].astype(
            jnp.bfloat16
        )


def match(e, idx, rows=512):
    n, genes = e.shape
    nl = genes // LANES
    return pl.pallas_call(
        match_kernel,
        grid_spec=pltpu.PrefetchScalarGridSpec(
            num_scalar_prefetch=1,
            grid=(n // rows,),
            in_specs=[pl.BlockSpec((n, genes), lambda b, i: (0, 0))],
            out_specs=[
                pl.BlockSpec((rows, genes), lambda b, i: (b, 0)),
                pl.BlockSpec((1, genes), lambda b, i: (0, 0)),
            ],
            scratch_shapes=[
                pltpu.VMEM((n * nl, LANES), jnp.float32),
                pltpu.VMEM((rows * nl, LANES), jnp.float32),
            ],
        ),
        out_shape=[
            jax.ShapeDtypeStruct((n, genes), jnp.bfloat16),
            jax.ShapeDtypeStruct((1, genes), jnp.float32),
        ],
        name="match",
    )(idx, e)


def fold_sums(xs, e_ref, c_ref, sums):
    p, l, q = sums
    for k, x_ref in enumerate(xs):
        x = x_ref[...]
        s = x.shape[1]
        p = p + dot32(x, e_ref[k * s : (k + 1) * s, :])
        l = l + dot32(x, c_ref[k * s : (k + 1) * s, :])
        f = x.astype(jnp.float32)
        f = f * f
        for j in range(s // LANES):
            q = q + f[:, j * LANES : (j + 1) * LANES]
    return p, l, q


def fold_kernel(*refs, pieces, fresh):
    xs = refs[:pieces]
    e_ref, c_ref = refs[pieces : pieces + 2]
    outs = refs[-3:]
    if fresh:
        sums = tuple(jnp.zeros(o.shape, jnp.float32) for o in outs)
    else:
        sums = tuple(r[...] for r in refs[pieces + 2 : pieces + 5])
    for o, v in zip(outs, fold_sums(xs, e_ref, c_ref, sums)):
        o[...] = v


def fold(xs, e, c, at, sums, tile=256):
    pieces = len(xs)
    width, s = xs[0].shape
    genes, covars = e.shape[1], c.shape[1]
    depth = pieces * s
    blk = at * s // depth
    assert blk * depth == at * s
    widths = (genes, covars, LANES)
    row = lambda w: pl.BlockSpec((tile, w), lambda i: (i, 0))
    in_specs = [row(s)] * pieces + [
        pl.BlockSpec((depth, genes), lambda i: (blk, 0)),
        pl.BlockSpec((depth, covars), lambda i: (blk, 0)),
    ]
    args = list(xs) + [e, c]
    aliases = {}
    if sums is not None:
        aliases = {pieces + 2 + k: k for k in range(3)}
        in_specs += [row(w) for w in widths]
        args += list(sums)
    return pl.pallas_call(
        functools.partial(fold_kernel, pieces=pieces, fresh=sums is None),
        grid=(width // tile,),
        in_specs=in_specs,
        out_specs=[row(w) for w in widths],
        out_shape=[jax.ShapeDtypeStruct((width, w), jnp.float32) for w in widths],
        input_output_aliases=aliases,
        name="fold",
    )(*args)


def finish_kernel(*refs, pieces, scale):
    xs = refs[:pieces]
    e_ref, c_ref, p_ref, l_ref, q_ref, d_ref, norm_ref = refs[pieces : pieces + 7]
    o_ref = refs[-1]
    genes = p_ref.shape[1]
    p, l, q = fold_sums(xs, e_ref, c_ref, (p_ref[...], l_ref[...], q_ref[...]))
    t = jnp.dot(
        l, d_ref[...], precision=lax.Precision.HIGHEST, preferred_element_type=jnp.float32
    )
    w = t[:, genes:]
    resid_norm = jnp.sum(q, axis=1, keepdims=True) - jnp.sum(w * w, axis=1, keepdims=True)
    resid_norm = jnp.maximum(resid_norm, 0.0)
    o_ref[...] = (
        scale
        * (p - t[:, :genes])
        * lax.rsqrt(resid_norm + epsilon)
        * lax.rsqrt(norm_ref[...] + epsilon)
    )


def finish(xs, e, c, at, sums, d, norm, scale, block, blocks, out, tile=256):
    pieces = len(xs)
    width, s = xs[0].shape
    genes, covars = e.shape[1], c.shape[1]
    depth = pieces * s
    blk = at * s // depth
    assert blk * depth == at * s
    row = lambda w: pl.BlockSpec((tile, w), lambda i: (i, 0))
    whole = lambda a: pl.BlockSpec(a.shape, lambda i: (0, 0))
    in_specs = [row(s)] * pieces + [
        pl.BlockSpec((depth, genes), lambda i: (blk, 0)),
        pl.BlockSpec((depth, covars), lambda i: (blk, 0)),
        row(genes),
        row(covars),
        row(LANES),
        whole(d),
        whole(norm),
    ]
    args = list(xs) + [e, c, *sums, d, norm]
    aliases = {}
    if out is not None:
        in_specs.append(pl.BlockSpec(memory_space=pl.ANY))
        aliases = {len(args): 0}
        args.append(out)
    steps = width // tile
    return pl.pallas_call(
        functools.partial(finish_kernel, pieces=pieces, scale=scale),
        grid=(steps,),
        in_specs=in_specs,
        out_specs=pl.BlockSpec((tile, genes), lambda i: (block * steps + i, 0)),
        out_shape=jax.ShapeDtypeStruct((blocks * width, genes), jnp.float32),
        input_output_aliases=aliases,
        name="finish",
    )(*args)


def ring_of(mesh):
    line = mesh.devices.reshape(mesh.shape["groups"], mesh.shape["samp"])[0]
    chips = line.shape[0] // 2
    plain = list(range(chips))
    spots = [tuple(getattr(line[2 * k], "coords", (0, 0, k))) for k in plain]
    wide = [a for a in range(3) if len({s[a] for s in spots}) > 1]
    if len(wide) == 2:
        short, long = sorted(wide, key=lambda a: len({s[a] for s in spots}))
        sides = sorted({s[short] for s in spots})
        if len(sides) == 2:
            up = sorted((k for k in plain if spots[k][short] == sides[0]), key=lambda k: spots[k][long])
            down = sorted((k for k in plain if spots[k][short] == sides[1]), key=lambda k: -spots[k][long])
            return up + down
    return plain


def local(ring, dosage, covariates, expression, block_index, expr_row):
    blocks = block_index.shape[0]
    samples = expr_row.shape[0]
    here, covars = covariates.shape
    genes = expression.shape[1]
    scale = math.sqrt(samples - covars - 1)
    chips = len(ring)
    half = chips // 2

    def shift(x, by):
        pairs = [
            (2 * ring[k] + core, 2 * ring[(k + by) % chips] + core)
            for k in range(chips)
            for core in range(2)
        ]
        return lax.ppermute(x, "samp", pairs)

    def swap(x):
        return lax.ppermute(x, "samp", [(k, k ^ 1) for k in range(2 * chips)])

    order = []
    for d in range(1, half):
        order += [d, -d]
    order += [0, half]

    mine = jnp.concatenate(
        [(shift(covariates, o) if o else covariates)[None] for o in order], axis=0
    )
    both = jnp.stack([mine, swap(mine)], axis=1)
    cov = both.reshape(samples, covars)

    me = lax.axis_index("samp")
    place = [0] * chips
    for k, chip in enumerate(ring):
        place[chip] = k
    spot = jnp.array(place, jnp.int32)[me // 2]
    chip = jnp.array(ring, jnp.int32)[(spot - jnp.array(order, jnp.int32)) % chips]
    core = jnp.stack([me % 2, 1 - me % 2])
    shard = (chip[:, None] * 2 + core[None, :]).reshape(-1)
    rows = jnp.take(expr_row.reshape(-1, here), shard, axis=0).reshape(-1)

    picks = [pick(dosage, block_index[b]) for b in range(blocks)]
    matched, panel_norm = match(expression, rows)

    gram = lax.dot_general(cov, cov, (((0,), (0,)), ((), ())), preferred_element_type=jnp.float32)
    cross = lax.dot_general(
        cov, matched, (((0,), (0,)), ((), ())), preferred_element_type=jnp.float32
    )
    factor = jnp.linalg.cholesky(gram)
    inverse = jax.scipy.linalg.solve_triangular(factor, jnp.eye(covars, dtype=jnp.float32), lower=True)
    high = functools.partial(jnp.dot, precision=lax.Precision.HIGHEST)
    slope = high(inverse.T, high(inverse, cross))
    back = jnp.concatenate(
        [slope, inverse.T, jnp.zeros((covars, LANES - covars % LANES), jnp.float32)], axis=1
    )

    out = None
    sums = [fold([p, swap(p)], matched, cov, 4 * half - 4, None) for p in picks]
    right = list(picks)
    left = list(picks)
    for d in range(1, half):
        for b in range(blocks):
            right[b] = shift(right[b], 1)
            left[b] = shift(left[b], -1)
            pieces = [right[b], swap(right[b]), left[b], swap(left[b])]
            sums[b] = fold(pieces, matched, cov, 4 * d - 4, sums[b])
    for b in range(blocks):
        last = shift(right[b], 1) if b % 2 == 0 else shift(left[b], -1)
        out = finish(
            [last, swap(last)], matched, cov, 4 * half - 2, sums[b], back, panel_norm, scale, b, blocks, out
        )
    return out


def solution(mesh):
    placed = (
        P(("groups", "samp"), None),
        P(("groups", "samp"), None),
        P("groups", "samp"),
        P("groups", None),
        P("groups"),
    )
    return jax.shard_map(
        functools.partial(local, ring_of(mesh)),
        mesh=mesh,
        in_specs=placed,
        out_specs=P("groups", "samp"),
        check_vma=False,
    )
```

```python
import functools
import math

import jax
import jax.numpy as jnp
from jax import lax
from jax.experimental import pallas as pl
from jax.experimental.pallas import tpu as pltpu
from jax.sharding import PartitionSpec as P


epsilon = 1e-06
LANES = 128
PARTS = 2


def dot32(a, b):
    return jnp.dot(a, b, preferred_element_type=jnp.float32)


def gather_rows(dst, src, idx_ref, base, rows, nl, unroll=32):
    def body(j, _):
        first = pl.multiple_of(j * unroll, unroll)
        for u in range(unroll):
            i = idx_ref[base + first + u]
            dst[pl.ds(pl.multiple_of((first + u) * nl, nl), nl), :] = src[
                pl.ds(pl.multiple_of(i * nl, nl), nl), :
            ]
        return 0

    lax.fori_loop(0, rows // unroll, body, 0)


def limit(mib):
    return pltpu.CompilerParams(vmem_limit_bytes=mib * 2**20)


def held(array):
    return pltpu.with_memory_space_constraint(array, pltpu.VMEM)


HELD = pl.BlockSpec(memory_space=pltpu.VMEM)


def pick_kernel(idx_ref, x_hbm, o_ref, x_ref, t_ref, g_ref, sems):
    rows, n = x_ref.shape
    nl = rows // LANES
    width = o_ref.shape[0]
    step = 1024
    copies = [
        pltpu.make_async_copy(x_hbm.at[:, pl.ds(k, step)], x_ref.at[:, pl.ds(k, step)], sems.at[j])
        for j, k in enumerate(range(0, n, step))
    ]
    for copy in copies:
        copy.start()
    for copy, k in zip(copies, range(0, n, step)):
        copy.wait()
        v = x_ref[:, k : k + step].astype(jnp.float32).T
        for l in range(nl):
            t_ref[pl.ds(k * nl + l, step, stride=nl), :] = v[:, l * LANES : (l + 1) * LANES]
    gather_rows(g_ref, t_ref, idx_ref, 0, width, nl)
    for l in range(nl):
        o_ref[:, l * LANES : (l + 1) * LANES] = g_ref[pl.ds(l, width, stride=nl), :].astype(
            jnp.bfloat16
        )


def pick(x, idx):
    rows, n = x.shape
    (width,) = idx.shape
    nl = rows // LANES
    return pl.pallas_call(
        pick_kernel,
        grid_spec=pltpu.PrefetchScalarGridSpec(
            num_scalar_prefetch=1,
            grid=(1,),
            in_specs=[pl.BlockSpec(memory_space=pltpu.HBM)],
            out_specs=pl.BlockSpec((width, rows), lambda b, i: (0, 0)),
            scratch_shapes=[
                pltpu.VMEM((rows, n), jnp.bfloat16),
                pltpu.VMEM((n * nl, LANES), jnp.float32),
                pltpu.VMEM((width * nl, LANES), jnp.float32),
                pltpu.SemaphoreType.DMA((n // 1024,)),
            ],
        ),
        out_shape=jax.ShapeDtypeStruct((width, rows), jnp.bfloat16),
        compiler_params=limit(20),
        name="pick",
    )(idx, x)


def match_kernel(idx_ref, table_ref, me_ref, e_hbm, o_ref, norm_ref, e_ref, f_ref, g_ref, sems, *, chips):
    n, genes = e_ref.shape
    nl = genes // LANES
    rows = n // (2 * chips)
    step = 512
    copies = [
        pltpu.make_async_copy(e_hbm.at[pl.ds(k, step), :], e_ref.at[pl.ds(k, step), :], sems.at[j])
        for j, k in enumerate(range(0, n, step))
    ]
    for copy in copies:
        copy.start()
    total = jnp.zeros((8, genes), jnp.float32)
    for copy, k in zip(copies, range(0, n, step)):
        copy.wait()
        v = e_ref[k : k + step, :].astype(jnp.float32)
        for l in range(nl):
            f_ref[pl.ds(k * nl + l, step, stride=nl), :] = v[:, l * LANES : (l + 1) * LANES]
        total = total + jnp.sum((v * v).reshape(step // 8, 8, genes), axis=0)
    norm_ref[...] = jnp.sum(total, axis=0, keepdims=True)

    me = me_ref[0]
    spot = table_ref[me // 2]

    def shard(k, _):
        far = k // chips
        place = lax.rem(spot - table_ref[2 * chips + k - far * chips] + 2 * chips, chips)
        core = lax.rem(me + far, 2)
        first = (2 * table_ref[chips + place] + core) * rows
        gather_rows(g_ref, f_ref, idx_ref, first, rows, nl)
        here = pl.ds(pl.multiple_of(k * rows, rows), rows)
        for l in range(nl):
            o_ref[here, l * LANES : (l + 1) * LANES] = g_ref[pl.ds(l, rows, stride=nl), :].astype(
                jnp.bfloat16
            )
        return 0

    lax.fori_loop(0, 2 * chips, shard, 0)


def match(e, idx, table, me, chips):
    n, genes = e.shape
    nl = genes // LANES
    rows = n // (2 * chips)
    return pl.pallas_call(
        functools.partial(match_kernel, chips=chips),
        grid_spec=pltpu.PrefetchScalarGridSpec(
            num_scalar_prefetch=3,
            grid=(1,),
            in_specs=[pl.BlockSpec(memory_space=pltpu.HBM)],
            out_specs=[HELD, pl.BlockSpec((1, genes), lambda b, *_: (0, 0))],
            scratch_shapes=[
                pltpu.VMEM((n, genes), jnp.bfloat16),
                pltpu.VMEM((n * nl, LANES), jnp.float32),
                pltpu.VMEM((rows * nl, LANES), jnp.float32),
                pltpu.SemaphoreType.DMA((n // 512,)),
            ],
        ),
        out_shape=[
            pltpu.VMEM((n, genes), jnp.bfloat16),
            jax.ShapeDtypeStruct((1, genes), jnp.float32),
        ],
        compiler_params=limit(16 * n // 4096 + 2),
        name="match",
    )(idx, table, me, e)


def fold_sums(xs, e_ref, mine, theirs, at, sums):
    p, l, q = sums
    half = len(xs) // 2
    n = e_ref.shape[0]
    for far, c in enumerate((mine, theirs)):
        parts = [r[...] for r in xs[far * half : (far + 1) * half]]
        x = parts[0] if half == 1 else jnp.concatenate(parts, axis=1)
        depth = x.shape[1]
        first = far * (n // 2) + at * (depth // half)
        p = p + dot32(x, e_ref[first : first + depth, :])
        l = l + lax.dot_general(
            x, c, (((1,), (1,)), ((), ())), preferred_element_type=jnp.float32
        )
        f = x.astype(jnp.float32)
        f = f * f
        for j in range(depth // LANES):
            q = q + f[:, j * LANES : (j + 1) * LANES]
    return p, l, q


def fold_kernel(*refs, pieces, at, fresh, tile):
    xs = refs[:pieces]
    e_ref, mine_ref, theirs_ref = refs[pieces : pieces + 3]
    outs = refs[-3:]
    here = pl.ds(pl.multiple_of(pl.program_id(0) * tile, tile), tile)
    if fresh:
        sums = tuple(jnp.zeros((tile, o.shape[1]), jnp.float32) for o in outs)
    else:
        sums = tuple(r[here, :] for r in refs[pieces + 3 : pieces + 6])
    for o, v in zip(outs, fold_sums(xs, e_ref, mine_ref[...], theirs_ref[...], at, sums)):
        o[here, :] = v


def fold(xs, e, cov, at, sums, tile=256):
    pieces = len(xs)
    width, s = xs[0].shape
    genes = e.shape[1]
    covars = cov[0].shape[0]
    depth = pieces // 2 * s
    blk = at * s // depth
    assert blk * depth == at * s
    widths = (genes, covars, LANES)
    in_specs = [pl.BlockSpec((tile, s), lambda i: (i, 0))] * pieces + [HELD]
    in_specs += [pl.BlockSpec((covars, depth), lambda i: (0, blk))] * 2
    args = list(xs) + [held(e), *cov]
    aliases = {}
    if sums is not None:
        aliases = {pieces + 3 + k: k for k in range(3)}
        in_specs += [HELD] * 3
        args += [held(a) for a in sums]
    return pl.pallas_call(
        functools.partial(fold_kernel, pieces=pieces, at=at, fresh=sums is None, tile=tile),
        grid=(width // tile,),
        in_specs=in_specs,
        out_specs=[HELD] * 3,
        out_shape=[pltpu.VMEM((width, w), jnp.float32) for w in widths],
        input_output_aliases=aliases,
        compiler_params=limit(20),
        name="fold",
    )(*args)


def thirds(a):
    high = a.astype(jnp.bfloat16)
    rest = a - high.astype(jnp.float32)
    mid = rest.astype(jnp.bfloat16)
    low = (rest - mid.astype(jnp.float32)).astype(jnp.bfloat16)
    return high, mid, low


def solve_kernel(mine_ref, theirs_ref, e_ref, o_ref):
    size = mine_ref.shape[0]
    n, genes = e_ref.shape
    pitch = o_ref.shape[0] // 6
    across = (((1,), (1,)), ((), ()))
    mine, theirs = mine_ref[...], theirs_ref[...]
    m = lax.dot_general(mine, mine, across, preferred_element_type=jnp.float32)
    m = m + lax.dot_general(theirs, theirs, across, preferred_element_type=jnp.float32)
    cross = dot32(mine, e_ref[: n // 2, :]) + dot32(theirs, e_ref[n // 2 :, :])
    line = lax.broadcasted_iota(jnp.int32, (size, size), 0)
    lane = lax.broadcasted_iota(jnp.int32, (size, size), 1)
    for k in range(size):
        below = line[:, :1] > k
        factor = jnp.where(below, m[:, k : k + 1] / m[k : k + 1, k : k + 1], 0.0)
        row = jnp.where(lane[:1] == k, 1.0, m[k : k + 1, :])
        m = jnp.where((lane == k) & (line > k), 0.0, m) - factor * row
    pivot = jnp.sum(jnp.where(lane == line, m, 0.0), axis=1, keepdims=True)
    inverse = jnp.where(lane < line, m, jnp.where(lane == line, 1.0, 0.0)) * lax.rsqrt(pivot)
    high = functools.partial(
        lax.dot_general, precision=lax.Precision.HIGHEST, preferred_element_type=jnp.float32
    )
    down = (((0,), (0,)), ((), ()))
    slope = high(inverse, high(inverse, cross, (((1,), (0,)), ((), ()))), down)
    o_ref[...] = jnp.zeros(o_ref.shape, jnp.bfloat16)
    for first, part in ((0, slope), (genes, inverse.T)):
        h, i, l = thirds(part)
        for k, term in enumerate((h, i, l, h, i, h)):
            o_ref[k * pitch : k * pitch + size, first : first + part.shape[1]] = term


def solve(cov, e):
    size = cov[0].shape[0]
    pitch = size + -size % LANES
    _, genes = e.shape
    whole = lambda a: pl.BlockSpec(a.shape, lambda i: (0, 0))
    table = jax.ShapeDtypeStruct((6 * pitch, genes + pitch), jnp.bfloat16)
    return pl.pallas_call(
        solve_kernel,
        grid=(1,),
        in_specs=[whole(cov[0]), whole(cov[1]), HELD],
        out_specs=whole(table),
        out_shape=table,
        compiler_params=limit(20),
        name="solve",
    )(*cov, held(e))


def finish_kernel(*refs, pieces, at, scale, start):
    xs = refs[:pieces]
    e_ref, mine_ref, theirs_ref, p_ref, l_ref, q_ref, d_ref, norm_ref = refs[pieces : pieces + 8]
    o_ref = refs[-1]
    tile, genes = o_ref.shape
    here = pl.ds(pl.multiple_of(start + pl.program_id(0) * tile, tile), tile)
    sums = tuple(r[here, :] for r in (p_ref, l_ref, q_ref))
    p, l, q = fold_sums(xs, e_ref, mine_ref[...], theirs_ref[...], at, sums)
    blank = -l.shape[1] % LANES
    if blank:
        l = jnp.concatenate([l, jnp.zeros((tile, blank), jnp.float32)], axis=1)
    h, i, o = thirds(l)
    t = dot32(jnp.concatenate([h, h, h, i, i, o], axis=1), d_ref[...])
    w = t[:, genes:]
    resid_norm = jnp.sum(q, axis=1, keepdims=True) - jnp.sum(w * w, axis=1, keepdims=True)
    resid_norm = jnp.maximum(resid_norm, 0.0)
    o_ref[...] = (
        (p - t[:, :genes])
        * (scale * lax.rsqrt(resid_norm + epsilon))
        * lax.rsqrt(norm_ref[...] + epsilon)
    )


def finish(xs, e, cov, at, sums, d, norm, scale, start, block, blocks, out, tile=256):
    pieces = len(xs)
    width = sums[0].shape[0]
    rows, s = xs[0].shape
    genes = e.shape[1]
    covars = cov[0].shape[0]
    depth = pieces // 2 * s
    blk = at * s // depth
    assert blk * depth == at * s
    whole = lambda a: pl.BlockSpec(a.shape, lambda i: (0, 0))
    in_specs = [pl.BlockSpec((tile, s), lambda i: (i, 0))] * pieces + [HELD]
    in_specs += [pl.BlockSpec((covars, depth), lambda i: (0, blk))] * 2
    in_specs += [HELD] * 3 + [whole(d), whole(norm)]
    args = list(xs) + [held(e), *cov, *(held(a) for a in sums), d, norm]
    aliases = {}
    if out is not None:
        in_specs.append(pl.BlockSpec(memory_space=pl.ANY))
        aliases = {len(args): 0}
        args.append(out)
    first = (block * width + start) // tile
    return pl.pallas_call(
        functools.partial(finish_kernel, pieces=pieces, at=at, scale=scale, start=start),
        grid=(rows // tile,),
        in_specs=in_specs,
        out_specs=pl.BlockSpec((tile, genes), lambda i: (first + i, 0)),
        out_shape=jax.ShapeDtypeStruct((blocks * width, genes), jnp.float32),
        input_output_aliases=aliases,
        compiler_params=limit(20),
        name="finish",
    )(*args)


def ring_of(mesh):
    line = mesh.devices.reshape(mesh.shape["groups"], mesh.shape["samp"])[0]
    chips = line.shape[0] // 2
    plain = list(range(chips))
    spots = [tuple(getattr(line[2 * k], "coords", (0, 0, k))) for k in plain]
    wide = [a for a in range(3) if len({s[a] for s in spots}) > 1]
    if len(wide) == 2:
        short, long = sorted(wide, key=lambda a: len({s[a] for s in spots}))
        sides = sorted({s[short] for s in spots})
        if len(sides) == 2:
            up = sorted((k for k in plain if spots[k][short] == sides[0]), key=lambda k: spots[k][long])
            down = sorted((k for k in plain if spots[k][short] == sides[1]), key=lambda k: -spots[k][long])
            return up + down
    return plain


def local(ring, dosage, covariates, expression, block_index, expr_row):
    blocks = block_index.shape[0]
    samples = expr_row.shape[0]
    here, covars = covariates.shape
    scale = math.sqrt(samples - covars - 1)
    chips = len(ring)
    half = chips // 2

    def shift(x, by):
        pairs = [
            (2 * ring[k] + core, 2 * ring[(k + by) % chips] + core)
            for k in range(chips)
            for core in range(2)
        ]
        return lax.ppermute(x, "samp", pairs)

    def swap(x):
        return lax.ppermute(x, "samp", [(k, k ^ 1) for k in range(2 * chips)])

    order = []
    for d in range(1, half):
        order += [d, -d]
    order += [0, half]

    known = {0: covariates.T}
    for d in range(1, half + 1):
        known[d] = shift(known[d - 1], 1)
        if d < half:
            known[-d] = shift(known[1 - d], -1)
    mine = jnp.concatenate([known[o] for o in order], axis=1)
    cov = (mine, swap(mine))

    place = [0] * chips
    for k, chip in enumerate(ring):
        place[chip] = k
    table = jnp.array(place + ring + order, jnp.int32)
    me = lax.axis_index("samp").reshape(1)

    dosage = pltpu.with_memory_space_constraint(dosage, pltpu.HBM)
    expression = pltpu.with_memory_space_constraint(expression, pltpu.HBM)
    picks = []
    for b in range(blocks):
        picks.append(pick(dosage, block_index[b]))
    matched, panel_norm = match(expression, expr_row, table, me, chips)
    back = solve(cov, matched)

    sums = []
    for b in range(blocks):
        other = swap(picks[b])
        sums.append(fold([picks[b], other], matched, cov, 2 * half - 2, None))
    right = list(picks)
    left = list(picks)
    for d in range(1, half):
        for b in range(blocks):
            right[b] = shift(right[b], 1)
            left[b] = shift(left[b], -1)
            near = swap(right[b])
            far = swap(left[b])
            pieces = [right[b], left[b], near, far]
            sums[b] = fold(pieces, matched, cov, 2 * d - 2, sums[b])
    width = picks[0].shape[0]
    rows = width // PARTS
    out = None
    for part in range(PARTS):
        for b in range(blocks):
            here = slice(part * rows, (part + 1) * rows)
            last = shift(right[b][here], 1) if b % 2 == 0 else shift(left[b][here], -1)
            other = swap(last)
            out = finish(
                [last, other], matched, cov, 2 * half - 1, sums[b], back, panel_norm,
                scale, part * rows, b, blocks, out,
            )
    return out


def solution(mesh):
    placed = (
        P(("groups", "samp"), None),
        P(("groups", "samp"), None),
        P("groups", "samp"),
        P("groups", None),
        P("groups"),
    )
    ring = ring_of(mesh)

    def body(*args):
        return local(ring, *args)

    return jax.shard_map(
        body, mesh=mesh, in_specs=placed, out_specs=P("groups", "samp"), check_vma=False
    )
```

```python
import functools
import math

import jax
import jax.numpy as jnp
from jax import lax
from jax.experimental import pallas as pl
from jax.experimental.pallas import tpu as pltpu
from jax.sharding import PartitionSpec as P


epsilon = 1e-06
LANES = 128
PARTS = 1


def dot32(a, b):
    return jnp.dot(a, b, preferred_element_type=jnp.float32)


def gather_rows(dst, src, entry, rows, nl, unroll=32):
    def body(j, _):
        first = pl.multiple_of(j * unroll, unroll)
        for u in range(unroll):
            i = entry(first, u)
            dst[pl.ds(pl.multiple_of((first + u) * nl, nl), nl), :] = src[
                pl.ds(pl.multiple_of(i * nl, nl), nl), :
            ]
        return 0

    lax.fori_loop(0, rows // unroll, body, 0)


def limit(mib):
    return pltpu.CompilerParams(vmem_limit_bytes=mib * 2**20)


def held(array):
    return pltpu.with_memory_space_constraint(array, pltpu.VMEM)


HELD = pl.BlockSpec(memory_space=pltpu.VMEM)


def pick_kernel(idx_ref, x_hbm, o_ref, x_ref, t_ref, g_ref, sems):
    rows, n = x_ref.shape
    nl = rows // LANES
    width = o_ref.shape[0]
    step = 1024
    copies = [
        pltpu.make_async_copy(x_hbm.at[:, pl.ds(k, step)], x_ref.at[:, pl.ds(k, step)], sems.at[j])
        for j, k in enumerate(range(0, n, step))
    ]
    for copy in copies:
        copy.start()
    for copy, k in zip(copies, range(0, n, step)):
        copy.wait()
        v = x_ref[:, k : k + step].T.astype(jnp.float32)
        for l in range(nl):
            t_ref[pl.ds(k * nl + l, step, stride=nl), :] = v[:, l * LANES : (l + 1) * LANES]
    gather_rows(g_ref, t_ref, lambda k, u: idx_ref[k + u], width, nl)
    for l in range(nl):
        o_ref[:, l * LANES : (l + 1) * LANES] = g_ref[pl.ds(l, width, stride=nl), :].astype(
            jnp.bfloat16
        )


def pick(x, idx):
    rows, n = x.shape
    (width,) = idx.shape
    nl = rows // LANES
    return pl.pallas_call(
        pick_kernel,
        grid_spec=pltpu.PrefetchScalarGridSpec(
            num_scalar_prefetch=1,
            grid=(1,),
            in_specs=[pl.BlockSpec(memory_space=pltpu.HBM)],
            out_specs=pl.BlockSpec((width, rows), lambda b, i: (0, 0)),
            scratch_shapes=[
                pltpu.VMEM((rows, n), jnp.bfloat16),
                pltpu.VMEM((n * nl, LANES), jnp.float32),
                pltpu.VMEM((width * nl, LANES), jnp.float32),
                pltpu.SemaphoreType.DMA((n // 1024,)),
            ],
        ),
        out_shape=jax.ShapeDtypeStruct((width, rows), jnp.bfloat16),
        compiler_params=limit(20),
        name="pick",
    )(idx, x)


def match_kernel(idx_ref, table_ref, me_ref, e_hbm, o_ref, norm_ref, e_ref, f_ref, g_ref, sems, *, chips):
    n, genes = e_ref.shape
    nl = genes // LANES
    rows = n // (2 * chips)
    step = 512
    copies = [
        pltpu.make_async_copy(e_hbm.at[pl.ds(k, step), :], e_ref.at[pl.ds(k, step), :], sems.at[j])
        for j, k in enumerate(range(0, n, step))
    ]
    for copy in copies:
        copy.start()
    total = jnp.zeros((8, genes), jnp.float32)
    for copy, k in zip(copies, range(0, n, step)):
        copy.wait()
        v = e_ref[k : k + step, :].astype(jnp.float32)
        for l in range(nl):
            f_ref[pl.ds(k * nl + l, step, stride=nl), :] = v[:, l * LANES : (l + 1) * LANES]
        total = total + jnp.sum((v * v).reshape(step // 8, 8, genes), axis=0)
    norm_ref[...] = jnp.sum(total, axis=0, keepdims=True)

    me = me_ref[0]
    spot = table_ref[me // 2]

    def shard(k, _):
        far = k // chips
        place = lax.rem(spot - table_ref[2 * chips + k - far * chips] + 2 * chips, chips)
        core = lax.rem(me + far, 2)
        first = (2 * table_ref[chips + place] + core) * rows
        gather_rows(g_ref, f_ref, lambda k, u: idx_ref[first + k + u], rows, nl)
        here = pl.ds(pl.multiple_of(k * rows, rows), rows)
        for l in range(nl):
            o_ref[here, l * LANES : (l + 1) * LANES] = g_ref[pl.ds(l, rows, stride=nl), :].astype(
                jnp.bfloat16
            )
        return 0

    lax.fori_loop(0, 2 * chips, shard, 0)


def match(e, idx, table, me, chips):
    n, genes = e.shape
    nl = genes // LANES
    rows = n // (2 * chips)
    return pl.pallas_call(
        functools.partial(match_kernel, chips=chips),
        grid_spec=pltpu.PrefetchScalarGridSpec(
            num_scalar_prefetch=3,
            grid=(1,),
            in_specs=[pl.BlockSpec(memory_space=pltpu.HBM)],
            out_specs=[HELD, pl.BlockSpec((1, genes), lambda b, *_: (0, 0))],
            scratch_shapes=[
                pltpu.VMEM((n, genes), jnp.bfloat16),
                pltpu.VMEM((n * nl, LANES), jnp.float32),
                pltpu.VMEM((rows * nl, LANES), jnp.float32),
                pltpu.SemaphoreType.DMA((n // 512,)),
            ],
        ),
        out_shape=[
            pltpu.VMEM((n, genes), jnp.bfloat16),
            jax.ShapeDtypeStruct((1, genes), jnp.float32),
        ],
        compiler_params=limit(16 * n // 4096 + 2),
        name="match",
    )(idx, table, me, e)


def both_halves(xs, e_ref, at):
    near = len(xs) // 2
    n = e_ref.shape[0]
    x = jnp.concatenate([r[...] for r in xs], axis=1)
    depth = x.shape[1] // 2
    first = at * (depth // near)
    rows = [e_ref[k + first : k + first + depth, :] for k in (0, n // 2)]
    return x, jnp.concatenate(rows, axis=0)


def loads_and_squares(x, mine, theirs, l, q):
    c = jnp.concatenate([mine, theirs], axis=1)
    l = l + lax.dot_general(x, c, (((1,), (1,)), ((), ())), preferred_element_type=jnp.float32)
    f = x.astype(jnp.float32)
    f = f * f
    for j in range(x.shape[1] // LANES):
        q = q + f[:, j * LANES : (j + 1) * LANES]
    return l, q


def fold_kernel(*refs, pieces, at, fresh, tile):
    xs = refs[:pieces]
    e_ref, mine_ref, theirs_ref = refs[pieces : pieces + 3]
    outs = refs[-3:]
    here = pl.ds(pl.multiple_of(pl.program_id(0) * tile, tile), tile)
    if fresh:
        p, l, q = (jnp.zeros((tile, o.shape[1]), jnp.float32) for o in outs)
    else:
        p, l, q = (r[here, :] for r in refs[pieces + 3 : pieces + 6])
    x, e = both_halves(xs, e_ref, at)
    outs[0][here, :] = p + dot32(x, e)
    outs[1][here, :], outs[2][here, :] = loads_and_squares(
        x, mine_ref[...], theirs_ref[...], l, q
    )


def fold(xs, e, at, cov, cat, sums, tile=512):
    pieces = len(xs)
    width, s = xs[0].shape
    genes = e.shape[1]
    covars = cov[0].shape[0]
    depth = pieces // 2 * s
    blk = cat * s // depth
    assert blk * depth == cat * s
    widths = (genes, covars, LANES)
    in_specs = [pl.BlockSpec((tile, s), lambda i: (i, 0))] * pieces + [HELD]
    in_specs += [pl.BlockSpec((covars, depth), lambda i: (0, blk))] * 2
    args = list(xs) + [held(e), *cov]
    aliases = {}
    if sums is not None:
        aliases = {pieces + 3 + k: k for k in range(3)}
        in_specs += [HELD] * 3
        args += [held(a) for a in sums]
    return pl.pallas_call(
        functools.partial(fold_kernel, pieces=pieces, at=at, fresh=sums is None, tile=tile),
        grid=(width // tile,),
        in_specs=in_specs,
        out_specs=[HELD] * 3,
        out_shape=[pltpu.VMEM((width, w), jnp.float32) for w in widths],
        input_output_aliases=aliases,
        compiler_params=limit(20),
        name="fold",
    )(*args)


def thirds(a):
    high = a.astype(jnp.bfloat16)
    rest = a - high.astype(jnp.float32)
    mid = rest.astype(jnp.bfloat16)
    low = (rest - mid.astype(jnp.float32)).astype(jnp.bfloat16)
    return high, mid, low


def solve_kernel(*refs):
    o_ref, e_ref = refs[-1], refs[-2]
    size = refs[0].shape[0]
    _, genes = e_ref.shape
    pitch = o_ref.shape[0] // 6
    across = (((1,), (1,)), ((), ()))
    m = jnp.zeros((size, size), jnp.float32)
    cross = jnp.zeros((size, genes), jnp.float32)
    first = 0
    for c_ref in refs[:-2]:
        c = c_ref[...]
        m = m + lax.dot_general(c, c, across, preferred_element_type=jnp.float32)
        cross = cross + dot32(c, e_ref[first : first + c.shape[1], :])
        first += c.shape[1]
    line = lax.broadcasted_iota(jnp.int32, (size, size), 0)
    lane = lax.broadcasted_iota(jnp.int32, (size, size), 1)
    for k in range(size):
        below = line[:, :1] > k
        factor = jnp.where(below, m[:, k : k + 1] / m[k : k + 1, k : k + 1], 0.0)
        row = jnp.where(lane[:1] == k, 1.0, m[k : k + 1, :])
        m = jnp.where((lane == k) & (line > k), 0.0, m) - factor * row
    pivot = jnp.sum(jnp.where(lane == line, m, 0.0), axis=1, keepdims=True)
    inverse = jnp.where(lane < line, m, jnp.where(lane == line, 1.0, 0.0)) * lax.rsqrt(pivot)
    high = functools.partial(
        lax.dot_general, precision=lax.Precision.HIGHEST, preferred_element_type=jnp.float32
    )
    down = (((0,), (0,)), ((), ()))
    slope = high(inverse, high(inverse, cross, (((1,), (0,)), ((), ()))), down)
    o_ref[...] = jnp.zeros(o_ref.shape, jnp.bfloat16)
    for first, part in ((0, -slope), (genes, inverse.T)):
        h, i, l = thirds(part)
        for k, term in enumerate((h, i, l, h, i, h)):
            o_ref[k * pitch : k * pitch + size, first : first + part.shape[1]] = term


def solve(covs, e):
    size = covs[0].shape[0]
    pitch = size + -size % LANES
    genes = e.shape[1]
    return pl.pallas_call(
        solve_kernel,
        grid=(1,),
        in_specs=[pl.BlockSpec(a.shape, lambda i: (0, 0)) for a in covs] + [HELD],
        out_specs=HELD,
        out_shape=pltpu.VMEM((6 * pitch, genes + pitch), jnp.bfloat16),
        compiler_params=limit(20),
        name="solve",
    )(*covs, held(e))


def finish_kernel(*refs, sides, at, scale, starts, first):
    p_ref, l_ref, q_ref, e_ref, mine_ref, theirs_ref, d_ref, norm_ref = refs[2 * sides : 2 * sides + 8]
    out_ref, o_ref, sems = refs[-3:]
    genes = o_ref.shape[1]
    tile = refs[0].shape[0]
    mine, theirs = mine_ref[...], theirs_ref[...]
    gene_scale = scale * lax.rsqrt(norm_ref[...] + epsilon)
    copies = []
    for k in range(sides):
        here = slice(starts[k], starts[k] + tile)
        x, e = both_halves(refs[2 * k : 2 * k + 2], e_ref, at)
        l, q = loads_and_squares(x, mine, theirs, l_ref[here, :], q_ref[here, :])
        blank = -l.shape[1] % LANES
        if blank:
            l = jnp.concatenate([l, jnp.zeros((tile, blank), jnp.float32)], axis=1)
        h, i, o = thirds(l)
        l = jnp.concatenate([h, h, h, i, i, o], axis=1)
        w = dot32(l, d_ref[:, genes:])
        resid_norm = jnp.sum(q, axis=1, keepdims=True) - jnp.sum(w * w, axis=1, keepdims=True)
        row_scale = lax.rsqrt(jnp.maximum(resid_norm, 0.0) + epsilon)
        p = p_ref[here, :] + dot32(
            jnp.concatenate([x, l], axis=1), jnp.concatenate([e, d_ref[:, :genes]], axis=0)
        )
        o_ref[k * tile : (k + 1) * tile, :] = p * row_scale * gene_scale
        copies.append(
            pltpu.make_async_copy(
                o_ref.at[pl.ds(k * tile, tile), :],
                out_ref.at[pl.ds(first + starts[k], tile), :],
                sems.at[k],
            )
        )
        copies[-1].start()
    for copy in copies:
        copy.wait()


def finish(pieces, starts, e, at, cov, sums, d, norm, scale, block, blocks, out):
    sides = len(pieces)
    width = sums[0].shape[0]
    tile, _ = pieces[0][0].shape
    genes = e.shape[1]
    whole = lambda a: pl.BlockSpec(a.shape, lambda i: (0, 0))
    args = [x for xs in pieces for x in xs]
    in_specs = [whole(x) for x in args] + [HELD] * 4 + [whole(c) for c in cov] + [HELD, whole(norm)]
    args += [*(held(a) for a in sums), held(e), *cov, held(d), norm]
    aliases = {}
    if out is not None:
        in_specs.append(pl.BlockSpec(memory_space=pltpu.HBM))
        aliases = {len(args): 0}
        args.append(out)
    return pl.pallas_call(
        functools.partial(
            finish_kernel,
            sides=sides,
            at=at,
            scale=scale,
            starts=starts,
            first=block * width,
        ),
        grid=(1,),
        in_specs=in_specs,
        out_specs=pl.BlockSpec(memory_space=pltpu.HBM),
        out_shape=jax.ShapeDtypeStruct((blocks * width, genes), jnp.float32),
        scratch_shapes=[
            pltpu.VMEM((sides * tile, genes), jnp.float32),
            pltpu.SemaphoreType.DMA((sides,)),
        ],
        input_output_aliases=aliases,
        compiler_params=limit(20),
        name="finish",
    )(*args)


def ring_of(mesh):
    line = mesh.devices.reshape(mesh.shape["groups"], mesh.shape["samp"])[0]
    chips = line.shape[0] // 2
    plain = list(range(chips))
    spots = [tuple(getattr(line[2 * k], "coords", (0, 0, k))) for k in plain]
    wide = [a for a in range(3) if len({s[a] for s in spots}) > 1]
    if len(wide) == 2:
        short, long = sorted(wide, key=lambda a: len({s[a] for s in spots}))
        sides = sorted({s[short] for s in spots})
        if len(sides) == 2:
            up = sorted((k for k in plain if spots[k][short] == sides[0]), key=lambda k: spots[k][long])
            down = sorted((k for k in plain if spots[k][short] == sides[1]), key=lambda k: -spots[k][long])
            return up + down
    return plain


def local(ring, dosage, covariates, expression, block_index, expr_row):
    blocks = block_index.shape[0]
    samples = expr_row.shape[0]
    _, covars = covariates.shape
    scale = math.sqrt(samples - covars - 1)
    chips = len(ring)
    half = chips // 2

    def shift(x, by):
        pairs = [
            (2 * ring[k] + core, 2 * ring[(k + by) % chips] + core)
            for k in range(chips)
            for core in range(2)
        ]
        return lax.ppermute(x, "samp", pairs)

    def swap(x):
        return lax.ppermute(x, "samp", [(k, k ^ 1) for k in range(2 * chips)])

    rounds = [[1, -1, 0]] + [[d, -d] for d in range(2, half)] + [[half]]
    order = sum(rounds, [])

    known = {0: covariates.T}
    for d in range(1, half + 1):
        known[d] = shift(known[d - 1], 1)
        if d < half:
            known[-d] = shift(known[1 - d], -1)
    covs = []
    for d, some in enumerate(rounds, 1):
        mine = jnp.concatenate([known[o] for o in some], axis=1)
        covs.append((mine, swap(mine)))

    place = [0] * chips
    for k, chip in enumerate(ring):
        place[chip] = k
    table = jnp.array(place + ring + order, jnp.int32)
    me = lax.axis_index("samp").reshape(1)

    dosage = pltpu.with_memory_space_constraint(dosage, pltpu.HBM)
    expression = pltpu.with_memory_space_constraint(expression, pltpu.HBM)
    picks = []
    for b in range(blocks):
        picks.append(pick(dosage, block_index[b]))
    matched, panel_norm = match(expression, expr_row, table, me, chips)
    back = solve([c[far] for far in range(2) for c in covs], matched)

    sums = []
    for b in range(blocks):
        other = swap(picks[b])
        sums.append(fold([picks[b], other], matched, 2, covs[0], 2, None))
    right = list(picks)
    left = list(picks)
    for d in range(1, half):
        for b in range(blocks):
            right[b] = shift(right[b], 1)
            left[b] = shift(left[b], -1)
            near = swap(right[b])
            far = swap(left[b])
            pieces = [right[b], left[b], near, far]
            if d == 1:
                sums[b] = fold(pieces, matched, 0, covs[0], 0, sums[b])
            else:
                sums[b] = fold(pieces, matched, 2 * d - 1, covs[d - 1], 0, sums[b])
    width = picks[0].shape[0]
    out = None
    for b in range(blocks):
        parts = parts_of(b, blocks)
        tile = width // (2 * parts)
        for part in range(parts):
            starts = [part * tile, width // 2 + part * tile]
            pieces = []
            for come, step, first in ((right, 1, starts[0]), (left, -1, starts[1])):
                last = shift(come[b][first : first + tile], step)
                pieces.append((last, swap(last)))
            out = finish(
                pieces, starts, matched, 2 * half - 1, covs[-1], sums[b], back, panel_norm,
                scale, b, blocks, out,
            )
    return out


def parts_of(b, blocks):
    return PARTS if b == blocks - 1 else 1


def solution(mesh):
    placed = (
        P(("groups", "samp"), None),
        P(("groups", "samp"), None),
        P("groups", "samp"),
        P("groups", None),
        P("groups"),
    )
    ring = ring_of(mesh)

    def body(*args):
        return local(ring, *args)

    return jax.shard_map(
        body, mesh=mesh, in_specs=placed, out_specs=P("groups", "samp"), check_vma=False
    )
```

```python
import functools
import math

import jax
import jax.numpy as jnp
from jax import lax
from jax.experimental import pallas as pl
from jax.experimental.pallas import tpu as pltpu
from jax.sharding import PartitionSpec as P


epsilon = 1e-06
LANES = 128
PARTS = 1


def dot32(a, b):
    return jnp.dot(a, b, preferred_element_type=jnp.float32)


def gather_rows(dst, src, entry, rows, nl, unroll=32):
    def body(j, _):
        first = pl.multiple_of(j * unroll, unroll)
        for u in range(unroll):
            i = entry(first, u)
            dst[pl.ds(pl.multiple_of((first + u) * nl, nl), nl), :] = src[
                pl.ds(pl.multiple_of(i * nl, nl), nl), :
            ]
        return 0

    lax.fori_loop(0, rows // unroll, body, 0)


def limit(mib):
    return pltpu.CompilerParams(vmem_limit_bytes=mib * 2**20)


def held(array):
    return pltpu.with_memory_space_constraint(array, pltpu.VMEM)


HELD = pl.BlockSpec(memory_space=pltpu.VMEM)


def pick_kernel(idx_ref, x_hbm, o_ref, x_ref, t_ref, g_ref, sems):
    rows, n = x_ref.shape
    nl = rows // LANES
    width = o_ref.shape[0]
    step = 1024
    copies = [
        pltpu.make_async_copy(x_hbm.at[:, pl.ds(k, step)], x_ref.at[:, pl.ds(k, step)], sems.at[j])
        for j, k in enumerate(range(0, n, step))
    ]
    for copy in copies:
        copy.start()
    for copy, k in zip(copies, range(0, n, step)):
        copy.wait()
        v = x_ref[:, k : k + step].T.astype(jnp.float32)
        for l in range(nl):
            t_ref[pl.ds(k * nl + l, step, stride=nl), :] = v[:, l * LANES : (l + 1) * LANES]
    gather_rows(g_ref, t_ref, lambda k, u: idx_ref[k + u], width, nl)
    for l in range(nl):
        o_ref[:, l * LANES : (l + 1) * LANES] = g_ref[pl.ds(l, width, stride=nl), :].astype(
            jnp.bfloat16
        )


def pick(x, idx):
    rows, n = x.shape
    (width,) = idx.shape
    nl = rows // LANES
    return pl.pallas_call(
        pick_kernel,
        grid_spec=pltpu.PrefetchScalarGridSpec(
            num_scalar_prefetch=1,
            grid=(1,),
            in_specs=[pl.BlockSpec(memory_space=pltpu.HBM)],
            out_specs=pl.BlockSpec((width, rows), lambda b, i: (0, 0)),
            scratch_shapes=[
                pltpu.VMEM((rows, n), jnp.bfloat16),
                pltpu.VMEM((n * nl, LANES), jnp.float32),
                pltpu.VMEM((width * nl, LANES), jnp.float32),
                pltpu.SemaphoreType.DMA((n // 1024,)),
            ],
        ),
        out_shape=jax.ShapeDtypeStruct((width, rows), jnp.bfloat16),
        compiler_params=limit(20),
        name="pick",
    )(idx, x)


def match_kernel(idx_ref, table_ref, me_ref, e_hbm, o_ref, norm_ref, e_ref, f_ref, g_ref, sems, *, chips):
    n, genes = e_ref.shape
    nl = genes // LANES
    rows = n // (2 * chips)
    step = 512
    copies = [
        pltpu.make_async_copy(e_hbm.at[pl.ds(k, step), :], e_ref.at[pl.ds(k, step), :], sems.at[j])
        for j, k in enumerate(range(0, n, step))
    ]
    for copy in copies:
        copy.start()
    total = jnp.zeros((8, genes), jnp.float32)
    for copy, k in zip(copies, range(0, n, step)):
        copy.wait()
        v = e_ref[k : k + step, :].astype(jnp.float32)
        for l in range(nl):
            f_ref[pl.ds(k * nl + l, step, stride=nl), :] = v[:, l * LANES : (l + 1) * LANES]
        total = total + jnp.sum((v * v).reshape(step // 8, 8, genes), axis=0)
    norm_ref[...] = jnp.sum(total, axis=0, keepdims=True)

    me = me_ref[0]
    spot = table_ref[me // 2]

    def shard(k, _):
        far = k // chips
        place = lax.rem(spot - table_ref[2 * chips + k - far * chips] + 2 * chips, chips)
        core = lax.rem(me + far, 2)
        first = (2 * table_ref[chips + place] + core) * rows
        gather_rows(g_ref, f_ref, lambda k, u: idx_ref[first + k + u], rows, nl)
        here = pl.ds(pl.multiple_of(k * rows, rows), rows)
        for l in range(nl):
            o_ref[here, l * LANES : (l + 1) * LANES] = g_ref[pl.ds(l, rows, stride=nl), :].astype(
                jnp.bfloat16
            )
        return 0

    lax.fori_loop(0, 2 * chips, shard, 0)


def match(e, idx, table, me, chips):
    n, genes = e.shape
    nl = genes // LANES
    rows = n // (2 * chips)
    return pl.pallas_call(
        functools.partial(match_kernel, chips=chips),
        grid_spec=pltpu.PrefetchScalarGridSpec(
            num_scalar_prefetch=3,
            grid=(1,),
            in_specs=[pl.BlockSpec(memory_space=pltpu.HBM)],
            out_specs=[HELD, pl.BlockSpec((1, genes), lambda b, *_: (0, 0))],
            scratch_shapes=[
                pltpu.VMEM((n, genes), jnp.bfloat16),
                pltpu.VMEM((n * nl, LANES), jnp.float32),
                pltpu.VMEM((rows * nl, LANES), jnp.float32),
                pltpu.SemaphoreType.DMA((n // 512,)),
            ],
        ),
        out_shape=[
            pltpu.VMEM((n, genes), jnp.bfloat16),
            jax.ShapeDtypeStruct((1, genes), jnp.float32),
        ],
        compiler_params=limit(16 * n // 4096 + 2),
        name="match",
    )(idx, table, me, e)


def both_halves(xs, e_ref, at):
    near = len(xs) // 2
    n = e_ref.shape[0]
    x = jnp.concatenate([r[...] for r in xs], axis=1)
    depth = x.shape[1] // 2
    first = at * (depth // near)
    rows = [e_ref[k + first : k + first + depth, :] for k in (0, n // 2)]
    return x, jnp.concatenate(rows, axis=0)


def loads_and_squares(x, mine, theirs, l, q):
    c = jnp.concatenate([mine, theirs], axis=1)
    l = l + lax.dot_general(x, c, (((1,), (1,)), ((), ())), preferred_element_type=jnp.float32)
    f = x.astype(jnp.float32)
    f = f * f
    for j in range(x.shape[1] // LANES):
        q = q + f[:, j * LANES : (j + 1) * LANES]
    return l, q


def fold_kernel(*refs, pieces, at, fresh, tile):
    xs = refs[:pieces]
    e_ref, mine_ref, theirs_ref = refs[pieces : pieces + 3]
    outs = refs[-3:]
    here = pl.ds(pl.multiple_of(pl.program_id(0) * tile, tile), tile)
    if fresh:
        p, l, q = (jnp.zeros((tile, o.shape[1]), jnp.float32) for o in outs)
    else:
        p, l, q = (r[here, :] for r in refs[pieces + 3 : pieces + 6])
    x, e = both_halves(xs, e_ref, at)
    outs[0][here, :] = p + dot32(x, e)
    outs[1][here, :], outs[2][here, :] = loads_and_squares(
        x, mine_ref[...], theirs_ref[...], l, q
    )


def fold(xs, e, at, cov, cat, sums, tile=512):
    pieces = len(xs)
    width, s = xs[0].shape
    genes = e.shape[1]
    covars = cov[0].shape[0]
    depth = pieces // 2 * s
    blk = cat * s // depth
    assert blk * depth == cat * s
    widths = (genes, covars, LANES)
    in_specs = [pl.BlockSpec((tile, s), lambda i: (i, 0))] * pieces + [HELD]
    in_specs += [pl.BlockSpec((covars, depth), lambda i: (0, blk))] * 2
    args = list(xs) + [held(e), *cov]
    aliases = {}
    if sums is not None:
        aliases = {pieces + 3 + k: k for k in range(3)}
        in_specs += [HELD] * 3
        args += [held(a) for a in sums]
    return pl.pallas_call(
        functools.partial(fold_kernel, pieces=pieces, at=at, fresh=sums is None, tile=tile),
        grid=(width // tile,),
        in_specs=in_specs,
        out_specs=[HELD] * 3,
        out_shape=[pltpu.VMEM((width, w), jnp.float32) for w in widths],
        input_output_aliases=aliases,
        compiler_params=limit(20),
        name="fold",
    )(*args)


def thirds(a):
    high = a.astype(jnp.bfloat16)
    rest = a - high.astype(jnp.float32)
    mid = rest.astype(jnp.bfloat16)
    low = (rest - mid.astype(jnp.float32)).astype(jnp.bfloat16)
    return high, mid, low


def solve_kernel(*refs):
    o_ref, e_ref = refs[-1], refs[-2]
    size = refs[0].shape[0]
    _, genes = e_ref.shape
    pitch = o_ref.shape[0] // 6
    across = (((1,), (1,)), ((), ()))
    m = jnp.zeros((size, size), jnp.float32)
    cross = jnp.zeros((size, genes), jnp.float32)
    first = 0
    for c_ref in refs[:-2]:
        c = c_ref[...]
        m = m + lax.dot_general(c, c, across, preferred_element_type=jnp.float32)
        cross = cross + dot32(c, e_ref[first : first + c.shape[1], :])
        first += c.shape[1]
    line = lax.broadcasted_iota(jnp.int32, (size, size), 0)
    lane = lax.broadcasted_iota(jnp.int32, (size, size), 1)
    for k in range(size):
        below = line[:, :1] > k
        factor = jnp.where(below, m[:, k : k + 1] / m[k : k + 1, k : k + 1], 0.0)
        row = jnp.where(lane[:1] == k, 1.0, m[k : k + 1, :])
        m = jnp.where((lane == k) & (line > k), 0.0, m) - factor * row
    pivot = jnp.sum(jnp.where(lane == line, m, 0.0), axis=1, keepdims=True)
    inverse = jnp.where(lane < line, m, jnp.where(lane == line, 1.0, 0.0)) * lax.rsqrt(pivot)
    high = functools.partial(
        lax.dot_general, precision=lax.Precision.HIGHEST, preferred_element_type=jnp.float32
    )
    down = (((0,), (0,)), ((), ()))
    slope = high(inverse, high(inverse, cross, (((1,), (0,)), ((), ()))), down)
    o_ref[...] = jnp.zeros(o_ref.shape, jnp.bfloat16)
    for first, part in ((0, -slope), (genes, inverse.T)):
        h, i, l = thirds(part)
        for k, term in enumerate((h, i, l, h, i, h)):
            o_ref[k * pitch : k * pitch + size, first : first + part.shape[1]] = term


def solve(covs, e):
    size = covs[0].shape[0]
    pitch = size + -size % LANES
    genes = e.shape[1]
    return pl.pallas_call(
        solve_kernel,
        grid=(1,),
        in_specs=[pl.BlockSpec(a.shape, lambda i: (0, 0)) for a in covs] + [HELD],
        out_specs=HELD,
        out_shape=pltpu.VMEM((6 * pitch, genes + pitch), jnp.bfloat16),
        compiler_params=limit(20),
        name="solve",
    )(*covs, held(e))


def finish_kernel(*refs, sides, at, scale, starts, first):
    p_ref, l_ref, q_ref, e_ref, mine_ref, theirs_ref, d_ref, norm_ref = refs[2 * sides : 2 * sides + 8]
    out_ref, o_ref, sems = refs[-3:]
    genes = o_ref.shape[1]
    tile = refs[0].shape[0]
    mine, theirs = mine_ref[...], theirs_ref[...]
    gene_scale = scale * lax.rsqrt(norm_ref[...] + epsilon)
    copies = []
    for k in range(sides):
        here = slice(starts[k], starts[k] + tile)
        x, e = both_halves(refs[2 * k : 2 * k + 2], e_ref, at)
        l, q = loads_and_squares(x, mine, theirs, l_ref[here, :], q_ref[here, :])
        blank = -l.shape[1] % LANES
        if blank:
            l = jnp.concatenate([l, jnp.zeros((tile, blank), jnp.float32)], axis=1)
        h, i, o = thirds(l)
        l = jnp.concatenate([h, h, h, i, i, o], axis=1)
        w = dot32(l, d_ref[:, genes:])
        resid_norm = jnp.sum(q, axis=1, keepdims=True) - jnp.sum(w * w, axis=1, keepdims=True)
        row_scale = lax.rsqrt(jnp.maximum(resid_norm, 0.0) + epsilon)
        p = p_ref[here, :] + dot32(
            jnp.concatenate([x, l], axis=1), jnp.concatenate([e, d_ref[:, :genes]], axis=0)
        )
        o_ref[k * tile : (k + 1) * tile, :] = p * row_scale * gene_scale
        copies.append(
            pltpu.make_async_copy(
                o_ref.at[pl.ds(k * tile, tile), :],
                out_ref.at[pl.ds(first + starts[k], tile), :],
                sems.at[k],
            )
        )
        copies[-1].start()
    for copy in copies:
        copy.wait()


def finish(pieces, starts, e, at, cov, sums, d, norm, scale, block, blocks, out):
    sides = len(pieces)
    width = sums[0].shape[0]
    tile, _ = pieces[0][0].shape
    genes = e.shape[1]
    whole = lambda a: pl.BlockSpec(a.shape, lambda i: (0, 0))
    args = [x for xs in pieces for x in xs]
    in_specs = [whole(x) for x in args] + [HELD] * 4 + [whole(c) for c in cov] + [HELD, whole(norm)]
    args += [*(held(a) for a in sums), held(e), *cov, held(d), norm]
    aliases = {}
    if out is not None:
        in_specs.append(pl.BlockSpec(memory_space=pltpu.HBM))
        aliases = {len(args): 0}
        args.append(out)
    return pl.pallas_call(
        functools.partial(
            finish_kernel,
            sides=sides,
            at=at,
            scale=scale,
            starts=starts,
            first=block * width,
        ),
        grid=(1,),
        in_specs=in_specs,
        out_specs=pl.BlockSpec(memory_space=pltpu.HBM),
        out_shape=jax.ShapeDtypeStruct((blocks * width, genes), jnp.float32),
        scratch_shapes=[
            pltpu.VMEM((sides * tile, genes), jnp.float32),
            pltpu.SemaphoreType.DMA((sides,)),
        ],
        input_output_aliases=aliases,
        compiler_params=limit(20),
        name="finish",
    )(*args)


def ring_of(mesh):
    line = mesh.devices.reshape(mesh.shape["groups"], mesh.shape["samp"])[0]
    chips = line.shape[0] // 2
    plain = list(range(chips))
    spots = [tuple(getattr(line[2 * k], "coords", (0, 0, k))) for k in plain]
    wide = [a for a in range(3) if len({s[a] for s in spots}) > 1]
    if len(wide) == 2:
        short, long = sorted(wide, key=lambda a: len({s[a] for s in spots}))
        sides = sorted({s[short] for s in spots})
        if len(sides) == 2:
            up = sorted((k for k in plain if spots[k][short] == sides[0]), key=lambda k: spots[k][long])
            down = sorted((k for k in plain if spots[k][short] == sides[1]), key=lambda k: -spots[k][long])
            return up + down
    return plain


def local(ring, dosage, covariates, expression, block_index, expr_row):
    blocks = block_index.shape[0]
    samples = expr_row.shape[0]
    _, covars = covariates.shape
    scale = math.sqrt(samples - covars - 1)
    chips = len(ring)
    half = chips // 2

    def shift(x, by):
        pairs = [
            (2 * ring[k] + core, 2 * ring[(k + by) % chips] + core)
            for k in range(chips)
            for core in range(2)
        ]
        return lax.ppermute(x, "samp", pairs)

    def swap(x):
        return lax.ppermute(x, "samp", [(k, k ^ 1) for k in range(2 * chips)])

    rounds = [[1, -1, 0]] + [[d, -d] for d in range(2, half)] + [[half]]
    order = sum(rounds, [])

    known = {0: covariates.T}
    for d in range(1, half + 1):
        known[d] = shift(known[d - 1], 1)
        if d < half:
            known[-d] = shift(known[1 - d], -1)
    covs = []
    for d, some in enumerate(rounds, 1):
        mine = jnp.concatenate([known[o] for o in some], axis=1)
        covs.append((mine, swap(mine)))

    place = [0] * chips
    for k, chip in enumerate(ring):
        place[chip] = k
    table = jnp.array(place + ring + order, jnp.int32)
    me = lax.axis_index("samp").reshape(1)

    dosage = pltpu.with_memory_space_constraint(dosage, pltpu.HBM)
    expression = pltpu.with_memory_space_constraint(expression, pltpu.HBM)
    picks = []
    for b in range(blocks):
        picks.append(pick(dosage, block_index[b]))
    matched, panel_norm = match(expression, expr_row, table, me, chips)
    back = solve([c[far] for far in range(2) for c in covs], matched)

    sums = []
    for b in range(blocks):
        other = swap(picks[b])
        sums.append(fold([picks[b], other], matched, 2, covs[0], 2, None))
    right = list(picks)
    left = list(picks)
    for d in range(1, half):
        for b in range(blocks):
            right[b] = shift(right[b], 1)
            left[b] = shift(left[b], -1)
            near = swap(right[b])
            far = swap(left[b])
            pieces = [right[b], left[b], near, far]
            if d == 1:
                sums[b] = fold(pieces, matched, 0, covs[0], 0, sums[b])
            else:
                sums[b] = fold(pieces, matched, 2 * d - 1, covs[d - 1], 0, sums[b])
    width = picks[0].shape[0]
    out = None
    for b in range(blocks):
        parts = parts_of()
        tile = width // (2 * parts)
        for part in range(parts):
            starts = [part * tile, width // 2 + part * tile]
            pieces = []
            for come, step, first in ((right, 1, starts[0]), (left, -1, starts[1])):
                last = shift(come[b][first : first + tile], step)
                pieces.append((last, swap(last)))
            out = finish(
                pieces, starts, matched, 2 * half - 1, covs[-1], sums[b], back, panel_norm,
                scale, b, blocks, out,
            )
    return out


def parts_of():
    return PARTS


def solution(mesh):
    placed = (
        P(("groups", "samp"), None),
        P(("groups", "samp"), None),
        P("groups", "samp"),
        P("groups", None),
        P("groups"),
    )
    ring = ring_of(mesh)

    def body(*args):
        return local(ring, *args)

    return jax.shard_map(
        body, mesh=mesh, in_specs=placed, out_specs=P("groups", "samp"), check_vma=False
    )
```

```python
import functools
import math

import jax
import jax.numpy as jnp
from jax import lax
from jax.experimental import pallas as pl
from jax.experimental.pallas import tpu as pltpu
from jax.sharding import PartitionSpec as P


epsilon = 1e-06
LANES = 128
PARTS = 1
FINISH_ROWS = 256


def dot32(a, b):
    return jnp.dot(a, b, preferred_element_type=jnp.float32)


def gather_rows(dst, src, entry, rows, nl, unroll=32):
    def body(j, _):
        first = pl.multiple_of(j * unroll, unroll)
        for u in range(unroll):
            i = entry(first, u)
            dst[pl.ds(pl.multiple_of((first + u) * nl, nl), nl), :] = src[
                pl.ds(pl.multiple_of(i * nl, nl), nl), :
            ]
        return 0

    lax.fori_loop(0, rows // unroll, body, 0)


def limit(mib):
    return pltpu.CompilerParams(vmem_limit_bytes=mib * 2**20)


def held(array):
    return pltpu.with_memory_space_constraint(array, pltpu.VMEM)


HELD = pl.BlockSpec(memory_space=pltpu.VMEM)


def pick_kernel(idx_ref, x_hbm, o_ref, x_ref, t_ref, g_ref, sems):
    rows, n = x_ref.shape
    nl = rows // LANES
    width = o_ref.shape[0]
    step = 1024
    copies = [
        pltpu.make_async_copy(x_hbm.at[:, pl.ds(k, step)], x_ref.at[:, pl.ds(k, step)], sems.at[j])
        for j, k in enumerate(range(0, n, step))
    ]
    for copy in copies:
        copy.start()
    for copy, k in zip(copies, range(0, n, step)):
        copy.wait()
        v = x_ref[:, k : k + step].T.astype(jnp.float32)
        for l in range(nl):
            t_ref[pl.ds(k * nl + l, step, stride=nl), :] = v[:, l * LANES : (l + 1) * LANES]
    gather_rows(g_ref, t_ref, lambda k, u: idx_ref[k + u], width, nl)
    for l in range(nl):
        o_ref[:, l * LANES : (l + 1) * LANES] = g_ref[pl.ds(l, width, stride=nl), :].astype(
            jnp.bfloat16
        )


def pick(x, idx):
    rows, n = x.shape
    (width,) = idx.shape
    nl = rows // LANES
    return pl.pallas_call(
        pick_kernel,
        grid_spec=pltpu.PrefetchScalarGridSpec(
            num_scalar_prefetch=1,
            grid=(1,),
            in_specs=[pl.BlockSpec(memory_space=pltpu.HBM)],
            out_specs=pl.BlockSpec((width, rows), lambda b, i: (0, 0)),
            scratch_shapes=[
                pltpu.VMEM((rows, n), jnp.bfloat16),
                pltpu.VMEM((n * nl, LANES), jnp.float32),
                pltpu.VMEM((width * nl, LANES), jnp.float32),
                pltpu.SemaphoreType.DMA((n // 1024,)),
            ],
        ),
        out_shape=jax.ShapeDtypeStruct((width, rows), jnp.bfloat16),
        compiler_params=limit(20),
        name="pick",
    )(idx, x)


def match_kernel(idx_ref, table_ref, me_ref, e_hbm, o_ref, norm_ref, e_ref, f_ref, g_ref, sems, *, chips):
    n, genes = e_ref.shape
    nl = genes // LANES
    rows = n // (2 * chips)
    step = 512
    copies = [
        pltpu.make_async_copy(e_hbm.at[pl.ds(k, step), :], e_ref.at[pl.ds(k, step), :], sems.at[j])
        for j, k in enumerate(range(0, n, step))
    ]
    for copy in copies:
        copy.start()
    total = jnp.zeros((8, genes), jnp.float32)
    for copy, k in zip(copies, range(0, n, step)):
        copy.wait()
        v = e_ref[k : k + step, :].astype(jnp.float32)
        for l in range(nl):
            f_ref[pl.ds(k * nl + l, step, stride=nl), :] = v[:, l * LANES : (l + 1) * LANES]
        total = total + jnp.sum((v * v).reshape(step // 8, 8, genes), axis=0)
    norm_ref[...] = jnp.sum(total, axis=0, keepdims=True)

    me = me_ref[0]
    spot = table_ref[me // 2]

    def shard(k, _):
        far = k // chips
        place = lax.rem(spot - table_ref[2 * chips + k - far * chips] + 2 * chips, chips)
        core = lax.rem(me + far, 2)
        first = (2 * table_ref[chips + place] + core) * rows
        gather_rows(g_ref, f_ref, lambda k, u: idx_ref[first + k + u], rows, nl)
        here = pl.ds(pl.multiple_of(k * rows, rows), rows)
        for l in range(nl):
            o_ref[here, l * LANES : (l + 1) * LANES] = g_ref[pl.ds(l, rows, stride=nl), :].astype(
                jnp.bfloat16
            )
        return 0

    lax.fori_loop(0, 2 * chips, shard, 0)


def match(e, idx, table, me, chips):
    n, genes = e.shape
    nl = genes // LANES
    rows = n // (2 * chips)
    return pl.pallas_call(
        functools.partial(match_kernel, chips=chips),
        grid_spec=pltpu.PrefetchScalarGridSpec(
            num_scalar_prefetch=3,
            grid=(1,),
            in_specs=[pl.BlockSpec(memory_space=pltpu.HBM)],
            out_specs=[HELD, pl.BlockSpec((1, genes), lambda b, *_: (0, 0))],
            scratch_shapes=[
                pltpu.VMEM((n, genes), jnp.bfloat16),
                pltpu.VMEM((n * nl, LANES), jnp.float32),
                pltpu.VMEM((rows * nl, LANES), jnp.float32),
                pltpu.SemaphoreType.DMA((n // 512,)),
            ],
        ),
        out_shape=[
            pltpu.VMEM((n, genes), jnp.bfloat16),
            jax.ShapeDtypeStruct((1, genes), jnp.float32),
        ],
        compiler_params=limit(16 * n // 4096 + 2),
        name="match",
    )(idx, table, me, e)


def both_halves(xs, e_ref, at):
    near = len(xs) // 2
    n = e_ref.shape[0]
    x = jnp.concatenate([r[...] for r in xs], axis=1)
    depth = x.shape[1] // 2
    first = at * (depth // near)
    rows = [e_ref[k + first : k + first + depth, :] for k in (0, n // 2)]
    return x, jnp.concatenate(rows, axis=0)


def loads_and_squares(x, mine, theirs, l, q):
    c = jnp.concatenate([mine, theirs], axis=1)
    l = l + lax.dot_general(x, c, (((1,), (1,)), ((), ())), preferred_element_type=jnp.float32)
    f = x.astype(jnp.float32)
    f = f * f
    for j in range(x.shape[1] // LANES):
        q = q + f[:, j * LANES : (j + 1) * LANES]
    return l, q


def fold_kernel(*refs, pieces, at, fresh, tile):
    xs = refs[:pieces]
    e_ref, mine_ref, theirs_ref = refs[pieces : pieces + 3]
    outs = refs[-3:]
    here = pl.ds(pl.multiple_of(pl.program_id(0) * tile, tile), tile)
    if fresh:
        p, l, q = (jnp.zeros((tile, o.shape[1]), jnp.float32) for o in outs)
    else:
        p, l, q = (r[here, :] for r in refs[pieces + 3 : pieces + 6])
    x, e = both_halves(xs, e_ref, at)
    outs[0][here, :] = p + dot32(x, e)
    outs[1][here, :], outs[2][here, :] = loads_and_squares(
        x, mine_ref[...], theirs_ref[...], l, q
    )


def fold(xs, e, at, cov, cat, sums, tile=512):
    pieces = len(xs)
    width, s = xs[0].shape
    genes = e.shape[1]
    covars = cov[0].shape[0]
    depth = pieces // 2 * s
    blk = cat * s // depth
    assert blk * depth == cat * s
    widths = (genes, covars, LANES)
    in_specs = [pl.BlockSpec((tile, s), lambda i: (i, 0))] * pieces + [HELD]
    in_specs += [pl.BlockSpec((covars, depth), lambda i: (0, blk))] * 2
    args = list(xs) + [held(e), *cov]
    aliases = {}
    if sums is not None:
        aliases = {pieces + 3 + k: k for k in range(3)}
        in_specs += [HELD] * 3
        args += [held(a) for a in sums]
    return pl.pallas_call(
        functools.partial(fold_kernel, pieces=pieces, at=at, fresh=sums is None, tile=tile),
        grid=(width // tile,),
        in_specs=in_specs,
        out_specs=[HELD] * 3,
        out_shape=[pltpu.VMEM((width, w), jnp.float32) for w in widths],
        input_output_aliases=aliases,
        compiler_params=limit(20),
        name="fold",
    )(*args)


def thirds(a):
    high = a.astype(jnp.bfloat16)
    rest = a - high.astype(jnp.float32)
    mid = rest.astype(jnp.bfloat16)
    low = (rest - mid.astype(jnp.float32)).astype(jnp.bfloat16)
    return high, mid, low


def solve_kernel(*refs):
    o_ref, e_ref = refs[-1], refs[-2]
    size = refs[0].shape[0]
    _, genes = e_ref.shape
    pitch = o_ref.shape[0] // 6
    across = (((1,), (1,)), ((), ()))
    m = jnp.zeros((size, size), jnp.float32)
    cross = jnp.zeros((size, genes), jnp.float32)
    first = 0
    for c_ref in refs[:-2]:
        c = c_ref[...]
        m = m + lax.dot_general(c, c, across, preferred_element_type=jnp.float32)
        cross = cross + dot32(c, e_ref[first : first + c.shape[1], :])
        first += c.shape[1]
    line = lax.broadcasted_iota(jnp.int32, (size, size), 0)
    lane = lax.broadcasted_iota(jnp.int32, (size, size), 1)
    for k in range(size):
        below = line[:, :1] > k
        factor = jnp.where(below, m[:, k : k + 1] / m[k : k + 1, k : k + 1], 0.0)
        row = jnp.where(lane[:1] == k, 1.0, m[k : k + 1, :])
        m = jnp.where((lane == k) & (line > k), 0.0, m) - factor * row
    pivot = jnp.sum(jnp.where(lane == line, m, 0.0), axis=1, keepdims=True)
    inverse = jnp.where(lane < line, m, jnp.where(lane == line, 1.0, 0.0)) * lax.rsqrt(pivot)
    high = functools.partial(
        lax.dot_general, precision=lax.Precision.HIGHEST, preferred_element_type=jnp.float32
    )
    down = (((0,), (0,)), ((), ()))
    slope = high(inverse, high(inverse, cross, (((1,), (0,)), ((), ()))), down)
    o_ref[...] = jnp.zeros(o_ref.shape, jnp.bfloat16)
    for first, part in ((0, -slope), (genes, inverse.T)):
        h, i, l = thirds(part)
        for k, term in enumerate((h, i, l, h, i, h)):
            o_ref[k * pitch : k * pitch + size, first : first + part.shape[1]] = term


def solve(covs, e):
    size = covs[0].shape[0]
    pitch = size + -size % LANES
    genes = e.shape[1]
    return pl.pallas_call(
        solve_kernel,
        grid=(1,),
        in_specs=[pl.BlockSpec(a.shape, lambda i: (0, 0)) for a in covs] + [HELD],
        out_specs=HELD,
        out_shape=pltpu.VMEM((6 * pitch, genes + pitch), jnp.bfloat16),
        compiler_params=limit(20),
        name="solve",
    )(*covs, held(e))


def finish_kernel(*refs, sides, at, scale, starts, first):
    p_ref, l_ref, q_ref, e_ref, mine_ref, theirs_ref, d_ref, norm_ref = refs[2 * sides : 2 * sides + 8]
    out_ref, o_ref, sems = refs[-3:]
    genes = o_ref.shape[1]
    whole = refs[0].shape[0]
    tile = min(whole, FINISH_ROWS)
    cuts = whole // tile
    mine, theirs = mine_ref[...], theirs_ref[...]
    gene_scale = scale * lax.rsqrt(norm_ref[...] + epsilon)
    copies = []
    for k in range(sides * cuts):
        side, cut = divmod(k, cuts)
        start = starts[side] + cut * tile
        here = slice(start, start + tile)
        pieces = [r.at[cut * tile : (cut + 1) * tile, :] for r in refs[2 * side : 2 * side + 2]]
        x, e = both_halves(pieces, e_ref, at)
        l, q = loads_and_squares(x, mine, theirs, l_ref[here, :], q_ref[here, :])
        blank = -l.shape[1] % LANES
        if blank:
            l = jnp.concatenate([l, jnp.zeros((tile, blank), jnp.float32)], axis=1)
        h, i, o = thirds(l)
        l = jnp.concatenate([h, h, h, i, i, o], axis=1)
        w = dot32(l, d_ref[:, genes:])
        resid_norm = jnp.sum(q, axis=1, keepdims=True) - jnp.sum(w * w, axis=1, keepdims=True)
        row_scale = lax.rsqrt(jnp.maximum(resid_norm, 0.0) + epsilon)
        p = p_ref[here, :] + dot32(
            jnp.concatenate([x, l], axis=1), jnp.concatenate([e, d_ref[:, :genes]], axis=0)
        )
        o_ref[k * tile : (k + 1) * tile, :] = p * row_scale * gene_scale
        copies.append(
            pltpu.make_async_copy(
                o_ref.at[pl.ds(k * tile, tile), :],
                out_ref.at[pl.ds(first + start, tile), :],
                sems.at[k],
            )
        )
        copies[-1].start()
    for copy in copies:
        copy.wait()


def finish(pieces, starts, e, at, cov, sums, d, norm, scale, block, blocks, out):
    sides = len(pieces)
    width = sums[0].shape[0]
    tile, _ = pieces[0][0].shape
    genes = e.shape[1]
    whole = lambda a: pl.BlockSpec(a.shape, lambda i: (0, 0))
    args = [x for xs in pieces for x in xs]
    in_specs = [whole(x) for x in args] + [HELD] * 4 + [whole(c) for c in cov] + [HELD, whole(norm)]
    args += [*(held(a) for a in sums), held(e), *cov, held(d), norm]
    aliases = {}
    if out is not None:
        in_specs.append(pl.BlockSpec(memory_space=pltpu.HBM))
        aliases = {len(args): 0}
        args.append(out)
    return pl.pallas_call(
        functools.partial(
            finish_kernel,
            sides=sides,
            at=at,
            scale=scale,
            starts=starts,
            first=block * width,
        ),
        grid=(1,),
        in_specs=in_specs,
        out_specs=pl.BlockSpec(memory_space=pltpu.HBM),
        out_shape=jax.ShapeDtypeStruct((blocks * width, genes), jnp.float32),
        scratch_shapes=[
            pltpu.VMEM((sides * tile, genes), jnp.float32),
            pltpu.SemaphoreType.DMA((sides * -(-tile // FINISH_ROWS),)),
        ],
        input_output_aliases=aliases,
        compiler_params=limit(20),
        name="finish",
    )(*args)


def ring_of(mesh):
    line = mesh.devices.reshape(mesh.shape["groups"], mesh.shape["samp"])[0]
    chips = line.shape[0] // 2
    plain = list(range(chips))
    spots = [tuple(getattr(line[2 * k], "coords", (0, 0, k))) for k in plain]
    wide = [a for a in range(3) if len({s[a] for s in spots}) > 1]
    if len(wide) == 2:
        short, long = sorted(wide, key=lambda a: len({s[a] for s in spots}))
        sides = sorted({s[short] for s in spots})
        if len(sides) == 2:
            up = sorted((k for k in plain if spots[k][short] == sides[0]), key=lambda k: spots[k][long])
            down = sorted((k for k in plain if spots[k][short] == sides[1]), key=lambda k: -spots[k][long])
            return up + down
    return plain


def local(ring, dosage, covariates, expression, block_index, expr_row):
    blocks = block_index.shape[0]
    samples = expr_row.shape[0]
    _, covars = covariates.shape
    scale = math.sqrt(samples - covars - 1)
    chips = len(ring)
    half = chips // 2

    def shift(x, by):
        pairs = [
            (2 * ring[k] + core, 2 * ring[(k + by) % chips] + core)
            for k in range(chips)
            for core in range(2)
        ]
        return lax.ppermute(x, "samp", pairs)

    def swap(x):
        return lax.ppermute(x, "samp", [(k, k ^ 1) for k in range(2 * chips)])

    rounds = [[1, -1, 0]] + [[d, -d] for d in range(2, half)] + [[half]]
    order = sum(rounds, [])

    known = {0: covariates.T}
    for d in range(1, half + 1):
        known[d] = shift(known[d - 1], 1)
        if d < half:
            known[-d] = shift(known[1 - d], -1)
    covs = []
    for d, some in enumerate(rounds, 1):
        mine = jnp.concatenate([known[o] for o in some], axis=1)
        covs.append((mine, swap(mine)))

    place = [0] * chips
    for k, chip in enumerate(ring):
        place[chip] = k
    table = jnp.array(place + ring + order, jnp.int32)
    me = lax.axis_index("samp").reshape(1)

    dosage = pltpu.with_memory_space_constraint(dosage, pltpu.HBM)
    expression = pltpu.with_memory_space_constraint(expression, pltpu.HBM)
    picks = []
    for b in range(blocks):
        picks.append(pick(dosage, block_index[b]))
    matched, panel_norm = match(expression, expr_row, table, me, chips)
    back = solve([c[far] for far in range(2) for c in covs], matched)

    sums = []
    for b in range(blocks):
        other = swap(picks[b])
        sums.append(fold([picks[b], other], matched, 2, covs[0], 2, None))
    right = list(picks)
    left = list(picks)
    for d in range(1, half):
        for b in range(blocks):
            right[b] = shift(right[b], 1)
            left[b] = shift(left[b], -1)
            near = swap(right[b])
            far = swap(left[b])
            pieces = [right[b], left[b], near, far]
            if d == 1:
                sums[b] = fold(pieces, matched, 0, covs[0], 0, sums[b])
            else:
                sums[b] = fold(pieces, matched, 2 * d - 1, covs[d - 1], 0, sums[b])
    width = picks[0].shape[0]
    out = None
    for b in range(blocks):
        parts = parts_of()
        tile = width // (2 * parts)
        for part in range(parts):
            starts = [part * tile, width // 2 + part * tile]
            pieces = []
            for come, step, first in ((right, 1, starts[0]), (left, -1, starts[1])):
                last = shift(come[b][first : first + tile], step)
                pieces.append((last, swap(last)))
            out = finish(
                pieces, starts, matched, 2 * half - 1, covs[-1], sums[b], back, panel_norm,
                scale, b, blocks, out,
            )
    return out


def parts_of():
    return PARTS


def solution(mesh):
    placed = (
        P(("groups", "samp"), None),
        P(("groups", "samp"), None),
        P("groups", "samp"),
        P("groups", None),
        P("groups"),
    )
    ring = ring_of(mesh)

    def body(*args):
        return local(ring, *args)

    return jax.shard_map(
        body, mesh=mesh, in_specs=placed, out_specs=P("groups", "samp"), check_vma=False
    )
```
